1024 devices in a mesh: comp: 2 (over core), blk: 512 (over y, z, x).
Axes of the slice: x: 8, y: 8, z: 8, core: 2. Of those that a mesh axis runs over, the one named last changes fastest.
Arguments:
- initial: float32 [2, 5, 4096, 2048], P('comp', None, 'blk'), may hold values from -3 to 3
- ice_forcing: float32 [5, 4096, 2048], P(None, 'blk'), may hold values from -2 to 4, as said below
- ocean_current: float32 [2, 4096, 2048], P(None, 'blk'), may hold values from -1 to 1
- ice_cover: int32 [4096, 2048], P('blk'), may hold values from 0 to 1, as said below
- targets: int32 [2, 4096, 2048], P(None, 'blk'), may hold values from 0 to 32767, as said below
- weights: int32 [2, 4096, 2048], P(None, 'blk'), may hold values from 1 to 4
Outputs:
- state_out: float32 [2, 5, 4096, 2048], P('comp', None, 'blk')
- coupled: float32 [2, 3, 4096, 2048], P('comp', None, 'blk')
The draws below stay inside these ranges and needn't reach their ends.
Inputs may be any that keep to these rules, and one draw needn't show every extreme that they name: `ice_forcing`: channel 0 (mass) lies in 0.5 to 4, channel 1 (strength) and channel 4 (melt rate) in 0.2 to 2, channels 2 and 3 (wind stress) in -2 to 2. `ice_cover`: the share of ice-covered cells differs from strip to strip of 8 rows. `targets`: an entry of an ice cell at row r of its strip names an ocean row of the window no earlier than r.
All inputs are finite; a program needn't handle non-finite values.
Results may differ from the reference program's by a relative error of at most 0.0003.
Values sent between devices are 32-bit elements; how exact they have to be, the bound alone decides.
No kernel may reach another device: no remote copies, remote signals or barrier semaphores. Data moves between devices by JAX's collectives and lax.ppermute only.
A program may use at most 128 MiB of HBM per device.

```python
import math
import jax
import jax.numpy as jnp
from jax import lax

CX = 8
NY = 2048
SUBCYCLES = 16
INTERSECTIONS = 2
NX = 4096


def smooth_field(key, channels):
    row_pos = jnp.arange(NX, dtype=jnp.float32)[None, :, None]
    col_pos = jnp.arange(NY, dtype=jnp.float32)[None, None, :]
    summed = jnp.zeros((channels, NX, NY), jnp.float32)
    for wave_index in range(3):
        wave_key = jax.random.fold_in(key, 100 + wave_index)
        picks = jax.random.uniform(wave_key, (3, channels), jnp.float32)
        row_length = jnp.exp(math.log(48.0) + (math.log(160.0) - math.log(48.0)) * picks[0])[:, None, None]
        col_length = jnp.exp(math.log(32.0) + (math.log(512.0) - math.log(32.0)) * picks[1])[:, None, None]
        summed = summed + jnp.sin(2.0 * math.pi * (row_pos / row_length + col_pos / col_length + picks[2][:, None, None]))
    return summed / 2.0


def draw_initial(key, part):
    smooth = smooth_field(jax.random.fold_in(key, 31), 10).reshape(2, 5, NX, NY)
    noise = jax.random.normal(jax.random.fold_in(key, 32), (2, 5, NX, NY), jnp.float32)
    values = 0.8 * smooth + 0.35 * noise
    return jnp.clip(values, -3.0, 3.0).astype(jnp.float32)


def draw_ice_forcing(key, part):
    shape = (NX, NY)
    keys = jax.random.split(key, 5)
    smooth = smooth_field(jax.random.fold_in(key, 51), 2)
    mass = jnp.exp(jax.random.uniform(keys[0], shape, jnp.float32, math.log(0.5), math.log(4.0)))
    strength = jnp.exp(jax.random.uniform(keys[1], shape, jnp.float32, math.log(0.2), math.log(2.0)))
    wind_x = jnp.clip(0.6 * smooth[0] + 0.3 * jax.random.normal(keys[2], shape, jnp.float32), -2.0, 2.0)
    wind_y = jnp.clip(0.6 * smooth[1] + 0.3 * jax.random.normal(keys[3], shape, jnp.float32), -2.0, 2.0)
    melt = jnp.exp(jax.random.uniform(keys[4], shape, jnp.float32, math.log(0.2), math.log(2.0)))
    return jnp.stack([mass, strength, wind_x, wind_y, melt]).astype(jnp.float32)


def draw_ocean_current(key, part):
    smooth = smooth_field(jax.random.fold_in(key, 41), 2)
    noise = jax.random.uniform(jax.random.fold_in(key, 42), (2, NX, NY), jnp.float32, -1.0, 1.0)
    along = 0.6 * jnp.tanh(3.0 * smooth[0]) + 0.35 * noise[0]
    sideways = 0.5 * smooth[1] + 0.4 * noise[1]
    return jnp.clip(jnp.stack([along, sideways]), -1.0, 1.0).astype(jnp.float32)


def draw_ice_cover(key, part):
    level = jnp.minimum(jax.random.randint(jax.random.fold_in(key, 11), (NX // CX,), 0, 24), 8)
    cells = jax.random.randint(jax.random.fold_in(key, 12), (NX, NY), 0, 8)
    strip = jnp.arange(NX, dtype=jnp.int32) // CX
    return (cells < level[strip][:, None]).astype(jnp.int32)


def draw_targets(key, part):
    offset = jax.random.randint(jax.random.fold_in(key, 21), (INTERSECTIONS, NX, NY), 0, CX + 1)
    jitter = jax.random.randint(jax.random.fold_in(key, 22), (INTERSECTIONS, NX, NY), -2, 3)
    local_row = (jnp.arange(NX, dtype=jnp.int32) % CX)[None, :, None]
    column = jnp.arange(NY, dtype=jnp.int32)[None, None, :]
    return ((local_row + offset) * NY + (column + jitter) % NY).astype(jnp.int32)


def with_ends(array, stream_key, least, high):
    place = [jax.random.randint(jax.random.fold_in(stream_key, axis), (), 0, length) for axis, length in enumerate(array.shape)]
    main_axis = array.shape.index(max(array.shape))
    beside = place[:main_axis] + [(place[main_axis] + 1) % array.shape[main_axis]] + place[main_axis + 1:]
    return array.at[tuple(place)].set(least).at[tuple(beside)].set(high)


def setup_inputs(seed: int = 0) -> dict:
    key_list = jax.random.split(jax.random.key(seed), 7)
    initial = draw_initial(jax.random.fold_in(key_list[6], 71), 0)
    ice_forcing = draw_ice_forcing(jax.random.fold_in(key_list[6], 71), 0)
    ocean_current = draw_ocean_current(jax.random.fold_in(key_list[6], 71), 0)
    ice_cover = draw_ice_cover(jax.random.fold_in(key_list[6], 71), 0)
    targets = draw_targets(jax.random.fold_in(key_list[6], 71), 0)
    weights = with_ends(jax.random.randint(key_list[5], (INTERSECTIONS, NX, NY), 1, 5), jax.random.fold_in(key_list[5], 1), 1, 4).astype(jnp.int32)
    return dict(initial=initial, ice_forcing=ice_forcing, ocean_current=ocean_current, ice_cover=ice_cover, targets=targets, weights=weights)


relax_rate = 0.5
ecc_sq = 4.0
delta_floor = 0.1
coriolis = 0.1
drag_coef = 1.0
inertia = 4.0
courant = 0.2
dilution = 0.5
weight_norm = 4.0
level_speed = (1.0, 0.8, 0.6, 0.45, 0.3)

def along_rows(field):
    return 0.5 * (field[..., 2:, :] - field[..., :-2, :])

def across(field):
    padded = jnp.pad(field, [(0, 0)] * (field.ndim - 1) + [(1, 1)])
    return 0.5 * (padded[..., 2:] - padded[..., :-2])

def ice_step(fields, forcing, current, covered):
    vel_x = fields[0]
    vel_y = fields[1]
    strain_d = along_rows(vel_x) + across(vel_y[1:-1])
    strain_t = along_rows(vel_x) - across(vel_y[1:-1])
    strain_s = across(vel_x[1:-1]) + along_rows(vel_y)
    delta = jnp.sqrt(strain_d * strain_d + (strain_t * strain_t + strain_s * strain_s) / ecc_sq + delta_floor * delta_floor)
    press = forcing[1, 1:-1] * covered[1:-1]
    sig_one = (fields[2, 1:-1] + relax_rate * press * (strain_d / delta - 1.0)) / (1.0 + relax_rate)
    sig_two = (fields[3, 1:-1] + relax_rate * press * strain_t / (ecc_sq * delta)) / (1.0 + relax_rate)
    sig_shear = (fields[4, 1:-1] + relax_rate * press * strain_s / (2.0 * ecc_sq * delta)) / (1.0 + relax_rate)
    sig_xx = 0.5 * (sig_one + sig_two)
    sig_yy = 0.5 * (sig_one - sig_two)
    force_x = along_rows(sig_xx) + across(sig_shear[1:-1])
    force_y = along_rows(sig_shear) + across(sig_yy[1:-1])
    beta = inertia * forcing[0, 2:-2]
    old_x = vel_x[2:-2]
    old_y = vel_y[2:-2]
    denom = beta + drag_coef
    new_x = covered[2:-2] * (beta * old_x + coriolis * beta * old_y + force_x + forcing[2, 2:-2] + drag_coef * current[0, 2:-2]) / denom
    new_y = covered[2:-2] * (beta * old_y - coriolis * beta * old_x + force_y + forcing[3, 2:-2] + drag_coef * current[1, 2:-2]) / denom
    return jnp.stack([new_x, new_y, sig_one[1:-1], sig_two[1:-1], sig_shear[1:-1]])

def ocean_step(tracer, current):
    speed = jnp.asarray(level_speed, jnp.float32)[:, None, None]
    centre = tracer[:, 2:-2]
    below = centre - tracer[:, 1:-3]
    above = tracer[:, 3:-1] - centre
    padded = jnp.pad(centre, ((0, 0), (0, 0), (1, 1)))
    left_diff = centre - padded[:, :, :-2]
    right_diff = padded[:, :, 2:] - centre
    speed_x = speed * current[0, 2:-2][None]
    speed_y = speed * current[1, 2:-2][None]
    change = jnp.maximum(speed_x, 0.0) * below + jnp.minimum(speed_x, 0.0) * above + jnp.maximum(speed_y, 0.0) * left_diff + jnp.minimum(speed_y, 0.0) * right_diff
    return centre - courant * change

def coupling_terms(fields, forcing, current, covered):
    stress_x = covered * drag_coef * (fields[0] - current[0])
    stress_y = covered * drag_coef * (fields[1] - current[1])
    fresh = forcing[4] * covered * jnp.sqrt(1.0 + fields[0] * fields[0] + fields[1] * fields[1])
    return jnp.stack([stress_x, stress_y, fresh])

def pad_rows(values):
    return jnp.pad(values, [(0, 0)] * (values.ndim - 2) + [(2, 2), (0, 0)])

def reference(initial, ice_forcing, ocean_current, ice_cover, targets, weights):
    covered = ice_cover.astype(jnp.float32)
    forcing_pad = pad_rows(ice_forcing)
    current_pad = pad_rows(ocean_current)
    cover_pad = pad_rows(covered)

    def one_turn(carry, unused):
        ice_fields, salinity, total = carry
        ice_fields = ice_step(pad_rows(ice_fields), forcing_pad, current_pad, cover_pad)
        salinity = ocean_step(pad_rows(salinity), current_pad)
        total = total + coupling_terms(ice_fields, ice_forcing, ocean_current, covered)
        return ((ice_fields, salinity, total), None)
    start = (initial[0], initial[1], jnp.zeros((3, NX, NY), jnp.float32))
    (ice_fields, salinity, total), unused = lax.scan(one_turn, start, None, length=SUBCYCLES)
    average = total / SUBCYCLES
    row_index = jnp.arange(NX, dtype=jnp.int32)[:, None]
    base = row_index // CX * (CX * NY)
    glob = (targets + base[None]) % (NX * NY)
    scaled = weights.astype(jnp.float32) / weight_norm
    flat_glob = glob.reshape(-1)

    def spread(single):
        return jax.ops.segment_sum((single[None] * scaled).reshape(-1), flat_glob, num_segments=NX * NY)
    flux = jax.vmap(spread)(average).reshape(3, NX, NY)
    salinity = jnp.concatenate([salinity[:1] - dilution * flux[2][None], salinity[1:]], axis=0)
    state_out = jnp.stack([ice_fields, salinity])
    coupled = jnp.stack([average, flux])
    return (state_out, coupled)
```

```python
import jax
import jax.numpy as jnp
from jax import lax
from jax.experimental import pallas as pl
from jax.experimental.pallas import tpu as pltpu
from jax.sharding import PartitionSpec as P

SUBCYCLES = 16
ICE_DEPTH = 4
OCEAN_DEPTH = 8
LANES = 128
PAD = 8
GROUP = 4

keep = 1.0 / 1.5
gain = 0.5 / 1.5
coriolis = 0.1
drag_coef = 1.0
inertia = 4.0
courant = 0.2
dilution = 0.5
weight_norm = 4.0
level_speed = (1.0, 0.8, 0.6, 0.45, 0.3)

VMEM = pl.BlockSpec(memory_space=pltpu.VMEM)
SMEM = pl.BlockSpec(memory_space=pltpu.SMEM)
LIMITED = pltpu.CompilerParams(vmem_limit_bytes=20 * 1024 * 1024)


def prep_kernel(flag, initial, forcing, current, cover, out):
    @pl.when(flag[0] == 0)
    def _():
        out[0] = initial[0, 0]
        out[1] = initial[0, 1]
        out[2] = initial[0, 2] + initial[0, 3]
        out[3] = initial[0, 2] - initial[0, 3]
        out[4] = 2.0 * initial[0, 4]
        covered = cover[...].astype(jnp.float32)
        out[5] = gain * forcing[1] * covered
        g = covered / (inertia * forcing[0] + drag_coef)
        out[6] = g
        out[7] = g * (forcing[2] + drag_coef * current[0])
        out[8] = g * (forcing[3] + drag_coef * current[1])

    @pl.when(flag[0] != 0)
    def _():
        for level in range(5):
            out[level] = initial[0, level]
        out[5] = current[0]
        out[6] = current[1]
        out[7] = jnp.zeros_like(current[0])
        out[8] = jnp.zeros_like(current[0])


def load_window(dst, dst_plane, src_plane, low, own, high, tiles, base):
    rows = own.shape[1]
    for part, ref in enumerate((low, own, high)):
        for c in range(tiles):
            dst[dst_plane, base[1] + c, pl.ds(base[0] + part * rows, rows), :] = ref[
                src_plane, :, c * LANES : (c + 1) * LANES
            ]


def make_round(first, last, ocean_active, rows, tiles):
    window = 3 * rows
    low_off = PAD

    def spans(margin):
        count = window - 2 * margin
        if count <= 8:
            return (8,)
        if count <= 16:
            return (4, 12)
        return (0, 8, 16)

    def kernel(*refs):
        refs = list(refs)
        flag = refs.pop(0)
        own, low, high = refs[:3]
        refs = refs[3:]
        if not first:
            stat, total_in = refs[:2]
            refs = refs[2:]
        if last:
            melt, current, cover = refs[:3]
            refs = refs[3:]
        if first:
            out, total, stat = refs[:3]
            refs = refs[3:]
        else:
            out, total = refs[:2]
            refs = refs[2:]
        field, other = refs

        lane = lax.broadcasted_iota(jnp.int32, (8, LANES), 1)
        at_first = lane == 0
        at_last = lane == LANES - 1
        zero_column = jnp.zeros((window + 2 * PAD, LANES), jnp.float32)

        def sides(ref, plane, column, row, cache):
            def rolled(c, shift):
                key = (plane, c, row, shift)
                if key not in cache:
                    tile = ref[plane, column[c], pl.ds(row, 8), :]
                    cache[key] = pltpu.roll(tile, shift, 1)
                return cache[key]

            def at(i):
                left = jnp.where(at_first, rolled(i, 1), rolled(i + 1, 1))
                right = jnp.where(at_last, rolled(i + 2, LANES - 1), rolled(i + 1, LANES - 1))
                return left, right

            return at

        def over_tiles(body):
            def step(group, carry):
                column = [group * GROUP + i for i in range(GROUP + 2)]
                body(group, column)
                return carry

            lax.fori_loop(0, tiles // GROUP, step, 0)

        def ice():
            if first:
                for plane in range(4):
                    load_window(stat, plane, 5 + plane, low, own, high, tiles, (0, 0))
                for part in range(3):
                    total[part] = jnp.zeros((rows, tiles * LANES), jnp.float32)
            else:
                for part in range(3):
                    total[part] = total_in[part]
            for plane in range(5):
                load_window(field, plane, plane, low, own, high, tiles, (low_off, 1))
                field[plane, 0] = zero_column
                field[plane, tiles + 1] = zero_column

            for turn in range(ICE_DEPTH):
                stress_spans = spans(2 * turn + 1)
                speed_spans = spans(2 * turn + 2)

                def stress(group, column):
                    for span in stress_spans:
                        row = span + low_off
                        cache = {}
                        side_x = sides(field, 0, column, row, cache)
                        side_y = sides(field, 1, column, row, cache)
                        for i in range(GROUP):
                            here = column[i + 1]
                            left_x, right_x = side_x(i)
                            left_y, right_y = side_y(i)
                            row_x = (
                                field[0, here, pl.ds(row + 1, 8), :]
                                - field[0, here, pl.ds(row - 1, 8), :]
                            )
                            row_y = (
                                field[1, here, pl.ds(row + 1, 8), :]
                                - field[1, here, pl.ds(row - 1, 8), :]
                            )
                            col_x = right_x - left_x
                            col_y = right_y - left_y
                            strain_d = row_x + col_y
                            strain_t = row_x - col_y
                            strain_s = col_x + row_y
                            quarter_t = 0.25 * strain_t
                            square = (
                                strain_d * strain_d
                                + quarter_t * strain_t
                                + 0.25 * (strain_s * strain_s)
                                + 0.04
                            )
                            press = stat[0, column[i], pl.ds(span, 8), :]
                            scaled = press * lax.rsqrt(square)
                            at = (here, pl.ds(row, 8), slice(None))
                            field[(2,) + at] = keep * field[(2,) + at] + (
                                scaled * (strain_d + quarter_t) - press
                            )
                            field[(3,) + at] = keep * field[(3,) + at] + (
                                scaled * (strain_d - quarter_t) - press
                            )
                            field[(4,) + at] = keep * field[(4,) + at] + scaled * (
                                0.25 * strain_s
                            )

                def speed(group, column):
                    for span in speed_spans:
                        row = span + low_off
                        cache = {}
                        side_q = sides(field, 4, column, row, cache)
                        side_m = sides(field, 3, column, row, cache)
                        for i in range(GROUP):
                            here = column[i + 1]
                            left_q, right_q = side_q(i)
                            left_m, right_m = side_m(i)
                            force_x = (
                                field[2, here, pl.ds(row + 1, 8), :]
                                - field[2, here, pl.ds(row - 1, 8), :]
                            ) + (right_q - left_q)
                            force_y = (
                                field[4, here, pl.ds(row + 1, 8), :]
                                - field[4, here, pl.ds(row - 1, 8), :]
                            ) + (right_m - left_m)
                            at = (here, pl.ds(row, 8), slice(None))
                            old_x = field[(0,) + at]
                            old_y = field[(1,) + at]
                            beside = (column[i], pl.ds(span, 8), slice(None))
                            g = stat[(1,) + beside]
                            held = jnp.where(g > 0.0, 1.0 - g, 0.0)
                            quarter = 0.25 * g
                            field[(0,) + at] = (
                                held * (old_x + coriolis * old_y)
                                + quarter * force_x
                                + stat[(2,) + beside]
                            )
                            field[(1,) + at] = (
                                held * (old_y - coriolis * old_x)
                                + quarter * force_y
                                + stat[(3,) + beside]
                            )
                    for i in range(GROUP):
                        here = column[i + 1]
                        new_x = field[0, here, pl.ds(rows + low_off, 8), :]
                        new_y = field[1, here, pl.ds(rows + low_off, 8), :]
                        lanes = pl.ds(pl.multiple_of(column[i] * LANES, LANES), LANES)
                        total[0, :, lanes] += new_x
                        total[1, :, lanes] += new_y
                        total[2, :, lanes] += jnp.sqrt(1.0 + new_x * new_x + new_y * new_y)

                over_tiles(stress)
                over_tiles(speed)

            for c in range(tiles):
                lanes = slice(c * LANES, (c + 1) * LANES)
                mine = [field[p, c + 1, low_off + rows : low_off + 2 * rows, :] for p in range(5)]
                if last:
                    mine[2:] = [
                        0.5 * (mine[2] + mine[3]),
                        0.5 * (mine[2] - mine[3]),
                        0.5 * mine[4],
                    ]
                    covered = cover[:, lanes].astype(jnp.float32)
                    total[0, :, lanes] = (
                        total[0, :, lanes] * (1.0 / SUBCYCLES) - covered * current[0, :, lanes]
                    )
                    total[1, :, lanes] = (
                        total[1, :, lanes] * (1.0 / SUBCYCLES) - covered * current[1, :, lanes]
                    )
                    total[2, :, lanes] = (
                        total[2, :, lanes] * (melt[0, :, lanes] * covered) * (1.0 / SUBCYCLES)
                    )
                for p in range(5):
                    out[p, :, lanes] = mine[p]

        def ocean():
            if first:
                for plane in range(2):
                    load_window(stat, plane, 5 + plane, low, own, high, tiles, (0, 0))
            if not ocean_active:
                out[...] = own[:5]
                return
            for plane in range(5):
                load_window(field, plane, plane, low, own, high, tiles, (low_off, 1))
                for ref in (field, other):
                    ref[plane, 0] = zero_column
                    ref[plane, tiles + 1] = zero_column

            for turn in range(OCEAN_DEPTH):
                source, target = (field, other) if turn % 2 == 0 else (other, field)
                row_spans = spans(turn + 1)

                def advect(group, column):
                    for span in row_spans:
                        row = span + low_off
                        pos_x, neg_x, pos_y, neg_y = [], [], [], []
                        for i in range(GROUP):
                            beside = (column[i], pl.ds(span, 8), slice(None))
                            ux = courant * stat[(0,) + beside]
                            uy = courant * stat[(1,) + beside]
                            pos_x.append(jnp.maximum(ux, 0.0))
                            neg_x.append(jnp.minimum(ux, 0.0))
                            pos_y.append(jnp.maximum(uy, 0.0))
                            neg_y.append(jnp.minimum(uy, 0.0))
                        for level in range(5):
                            side = sides(source, level, column, row, {})
                            for i in range(GROUP):
                                here = column[i + 1]
                                left, right = side(i)
                                centre = source[level, here, pl.ds(row, 8), :]
                                below = source[level, here, pl.ds(row - 1, 8), :]
                                above = source[level, here, pl.ds(row + 1, 8), :]
                                change = (
                                    pos_x[i] * (centre - below)
                                    + neg_x[i] * (above - centre)
                                    + pos_y[i] * (centre - left)
                                    + neg_y[i] * (right - centre)
                                )
                                if level:
                                    change = level_speed[level] * change
                                target[level, here, pl.ds(row, 8), :] = centre - change

                over_tiles(advect)

            done = field if OCEAN_DEPTH % 2 == 0 else other
            for p in range(5):
                for c in range(tiles):
                    out[p, :, c * LANES : (c + 1) * LANES] = done[
                        p, c + 1, low_off + rows : low_off + 2 * rows, :
                    ]

        @pl.when(flag[0] == 0)
        def _():
            ice()

        @pl.when(flag[0] != 0)
        def _():
            ocean()

    return kernel


HIGH = 64
WIDE = 256


def scatter_half(half, values, targets, weights, out, left, right, sums):
    rows = values.shape[1]
    columns = values.shape[2]
    groups = columns // WIDE
    spots = rows * groups
    sums[...] = jnp.zeros_like(sums)
    high_at = lax.broadcasted_iota(jnp.int32, (spots, columns), 0).astype(jnp.bfloat16)
    low_at = lax.broadcasted_iota(jnp.int32, (WIDE, columns), 0).astype(jnp.bfloat16)
    zero = jnp.zeros((), jnp.bfloat16)
    one = jnp.ones((), jnp.bfloat16)

    def step(turn, carry):
        entry = turn // rows
        row = turn % rows
        spot = targets[entry, pl.ds(row, 1), :]
        scale = weights[entry, pl.ds(row, 1), :].astype(jnp.float32) / weight_norm
        low = jnp.bitwise_and(spot, WIDE - 1)
        high = jnp.right_shift(spot, 8) - half * spots
        inside = jnp.logical_and(high >= 0, high < spots)
        place = jnp.bitwise_and(high, groups - 1) * rows + high // groups
        place = jnp.where(inside, place, -1)
        low = low.astype(jnp.float32).astype(jnp.bfloat16)
        place = place.astype(jnp.float32).astype(jnp.bfloat16)
        right[...] = jnp.where(low_at == low, one, zero)
        hit = high_at == place
        for channel in range(3):
            value = values[channel, pl.ds(row, 1), :] * scale
            coarse = value.astype(jnp.bfloat16)
            fine = (value - coarse.astype(jnp.float32)).astype(jnp.bfloat16)
            left[2 * channel * spots : (2 * channel + 1) * spots, :] = jnp.where(hit, coarse, zero)
            left[(2 * channel + 1) * spots : (2 * channel + 2) * spots, :] = jnp.where(
                hit, fine, zero
            )
        sums[...] += lax.dot_general(
            left[...],
            right[...],
            (((1,), (1,)), ((), ())),
            preferred_element_type=jnp.float32,
        )
        return carry

    lax.fori_loop(0, 2 * rows, step, 0)
    for channel in range(3):
        for g in range(groups):
            first = 2 * channel * spots + g * rows
            second = first + spots
            out[channel, :, g * WIDE : (g + 1) * WIDE] = (
                sums[first : first + rows, :] + sums[second : second + rows, :]
            )


def upper_kernel(flag, average, targets, weights, out, left, right, sums):
    @pl.when(flag[0] == 0)
    def _():
        scatter_half(1, average, targets, weights, out, left, right, sums)


def lower_kernel(flag, average, targets, weights, out, left, right, sums):
    @pl.when(flag[0] != 0)
    def _():
        scatter_half(0, average, targets, weights, out, left, right, sums)


def final_kernel(flag, fields, average, lower, upper, state, coupled):
    @pl.when(flag[0] == 0)
    def _():
        state[0] = fields[...]
        coupled[0] = average[...]

    @pl.when(flag[0] != 0)
    def _():
        flux = lower[...] + upper[...]
        coupled[0] = flux
        state[0, 0] = fields[0] - dilution * flux[2]
        state[0, 1:] = fields[1:]


def body(initial, ice_forcing, ocean_current, ice_cover, targets, weights):
    rows, columns = initial.shape[2:]
    tiles = columns // LANES
    strips = lax.axis_size("blk")
    flag = lax.axis_index("comp").astype(jnp.int32).reshape(1)
    both = ("comp", "blk")

    def moved(value, kinds, step):
        pairs = [
            (kind * strips + b, kind * strips + b + step)
            for kind in kinds
            for b in range(strips)
            if 0 <= b + step < strips
        ]
        return lax.ppermute(value, both, pairs)

    def shape(*dims):
        return pltpu.VMEM(dims, jnp.float32)

    def held(*values):
        return [pltpu.with_memory_space_constraint(value, pltpu.VMEM) for value in values]

    block = pl.pallas_call(
        prep_kernel,
        compiler_params=LIMITED,
        out_shape=shape(9, rows, columns),
        in_specs=[SMEM] + [VMEM] * 4,
        out_specs=VMEM,
    )(flag, initial, ice_forcing, ocean_current, ice_cover)

    rounds = SUBCYCLES // ICE_DEPTH
    each = OCEAN_DEPTH // ICE_DEPTH
    window = 3 * rows
    stat = total = None
    for turn in range(rounds):
        first, last = turn == 0, turn == rounds - 1
        active = turn % each == 0
        kinds = (0, 1) if active else (0,)
        low = moved(block, kinds, 1)
        high = moved(block, kinds, -1)
        operands = [flag, block, low, high]
        outs = [shape(5, rows, columns), shape(3, rows, columns)]
        if not first:
            operands += [stat, total]
        if last:
            operands += [ice_forcing[4:], ocean_current, ice_cover]
        if first:
            outs.append(shape(4, tiles, window, LANES))
        done = pl.pallas_call(
            make_round(first, last, active, rows, tiles),
            compiler_params=LIMITED,
            out_shape=outs,
            in_specs=[SMEM] + [VMEM] * (len(operands) - 1),
            out_specs=[VMEM] * len(outs),
            scratch_shapes=[pltpu.VMEM((5, tiles + 2, window + 2 * PAD, LANES), jnp.float32)] * 2,
        )(flag, *held(*operands[1:]))
        block, total = done[:2]
        if first:
            stat = done[2]

    average = total
    scatter_scratch = [
        pltpu.VMEM((6 * rows * columns // WIDE, columns), jnp.bfloat16),
        pltpu.VMEM((WIDE, columns), jnp.bfloat16),
        pltpu.VMEM((6 * rows * columns // WIDE, WIDE), jnp.float32),
    ]

    def scattered(kernel, values):
        return pl.pallas_call(
            kernel,
            compiler_params=LIMITED,
            out_shape=shape(3, rows, columns),
            in_specs=[SMEM] + [VMEM] * 3,
            out_specs=VMEM,
            scratch_shapes=scatter_scratch,
        )(flag, *held(values, targets, weights))

    received = lax.ppermute(average, both, [(b, strips + b) for b in range(strips)])
    upper = scattered(upper_kernel, average)
    beyond = lax.ppermute(upper, both, [(b, strips + (b + 1) % strips) for b in range(strips)])
    lower = scattered(lower_kernel, received)
    return tuple(
        pl.pallas_call(
            final_kernel,
            compiler_params=LIMITED,
            out_shape=[
                jax.ShapeDtypeStruct((1, 5, rows, columns), jnp.float32),
                jax.ShapeDtypeStruct((1, 3, rows, columns), jnp.float32),
            ],
            in_specs=[SMEM] + [VMEM] * 4,
            out_specs=[VMEM] * 2,
        )(flag, *held(block, average, lower, beyond))
    )


def solution(mesh):
    placed = (
        P("comp", None, "blk", None),
        P(None, "blk", None),
        P(None, "blk", None),
        P("blk", None),
        P(None, "blk", None),
        P(None, "blk", None),
    )
    return jax.shard_map(
        body,
        mesh=mesh,
        in_specs=placed,
        out_specs=(P("comp", None, "blk", None), P("comp", None, "blk", None)),
        check_vma=False,
    )
```

```python
from functools import partial

import jax
import jax.numpy as jnp
from jax import lax
from jax.experimental import pallas as pl
from jax.experimental.pallas import tpu as pltpu
from jax.sharding import PartitionSpec as P

SUBCYCLES = 16
ICE_DEPTH = 4
OCEAN_DEPTH = 8
LANES = 128
PAD = 8
GROUP = 16
OCEAN_DELAY = 12000

keep = 1.0 / 1.5
gain = 0.5 / 1.5
coriolis = 0.1
drag_coef = 1.0
inertia = 4.0
courant = 0.2
dilution = 0.5
weight_norm = 4.0
level_speed = (1.0, 0.8, 0.6, 0.45, 0.3)

VMEM = pl.BlockSpec(memory_space=pltpu.VMEM)
SMEM = pl.BlockSpec(memory_space=pltpu.SMEM)
LIMITED = pltpu.CompilerParams(vmem_limit_bytes=20 * 1024 * 1024)


def prep_kernel(strips, flag, *refs):
    sources, out, (initial, forcing, current, cover), arrived = refs[:4], refs[4], refs[5:9], refs[9]
    copies = [
        pltpu.make_async_copy(source, target, arrived.at[i])
        for i, (source, target) in enumerate(zip(sources, (initial, forcing, current, cover)))
    ]
    for copy in copies:
        copy.start()
    for copy in copies:
        copy.wait()

    @pl.when(flag[0] < strips)
    def _():
        out[0] = initial[0, 0]
        out[1] = initial[0, 1]
        out[2] = initial[0, 2] + initial[0, 3]
        out[3] = initial[0, 2] - initial[0, 3]
        out[4] = 2.0 * initial[0, 4]
        covered = cover[...].astype(jnp.float32)
        out[5] = gain * forcing[1] * covered
        g = covered / (inertia * forcing[0] + drag_coef)
        out[6] = g
        out[7] = g * (forcing[2] + drag_coef * current[0])
        out[8] = g * (forcing[3] + drag_coef * current[1])

    @pl.when(flag[0] >= strips)
    def _():
        pl.delay(OCEAN_DELAY)
        for level in range(5):
            out[level] = initial[0, level]
        out[5] = current[0]
        out[6] = current[1]
        out[7] = jnp.zeros_like(current[0])
        out[8] = jnp.zeros_like(current[0])


def load_strip(dst, dst_plane, src, src_plane, part, tiles, base):
    rows = src.shape[1]
    for c in range(tiles):
        dst[dst_plane, base[1] + c, pl.ds(base[0] + part * rows, rows), :] = src[
            src_plane, :, c * LANES : (c + 1) * LANES
        ]


def make_round(strips, first, last, ocean_active, rows, tiles):
    window = 3 * rows
    low_off = PAD

    def spans(margin):
        count = window - 2 * margin
        if count <= 8:
            return (8,)
        if count <= 16:
            return (4, 12)
        return (0, 8, 16)

    def kernel(*refs):
        refs = list(refs)
        flag = refs.pop(0)
        own, near, far = refs[:3]
        refs = refs[3:]
        if first:
            targets, weights = refs[:2]
        else:
            stat, total_in = refs[:2]
        refs = refs[2:]
        if last:
            melt, current, cover = refs[:3]
            refs = refs[3:]
        if first:
            out, total, stat, links = refs[:4]
            refs = refs[4:]
        else:
            out, total = refs[:2]
            refs = refs[2:]
        field, other = refs

        lane = lax.broadcasted_iota(jnp.int32, (8, LANES), 1)
        at_first = lane == 0
        at_last = lane == LANES - 1
        odd = jnp.bitwise_and(flag[0], 1) == 1

        def load_windows(dst, planes, base):
            def halo(low, high):
                for plane, source in planes:
                    load_strip(dst, plane, low, source, 0, tiles, base)
                    load_strip(dst, plane, high, source, 2, tiles, base)

            for plane, source in planes:
                load_strip(dst, plane, own, source, 1, tiles, base)
            pl.when(odd)(lambda: halo(near, far))
            pl.when(jnp.logical_not(odd))(lambda: halo(far, near))

        zero_column = jnp.zeros((window + 2 * PAD, LANES), jnp.float32)

        def sides(ref, plane, column, row, cache):
            def rolled(c, shift):
                key = (plane, c, row, shift)
                if key not in cache:
                    tile = ref[plane, column[c], pl.ds(row, 8), :]
                    cache[key] = pltpu.roll(tile, shift, 1)
                return cache[key]

            def at(i):
                left = jnp.where(at_first, rolled(i, 1), rolled(i + 1, 1))
                right = jnp.where(at_last, rolled(i + 2, LANES - 1), rolled(i + 1, LANES - 1))
                return left, right

            return at

        def over_tiles(body):
            def step(group, carry):
                column = [group * GROUP + i for i in range(GROUP + 2)]
                body(group, column)
                return carry

            lax.fori_loop(0, tiles // GROUP, step, 0)

        def ice():
            if first:
                load_windows(stat, [(plane, 5 + plane) for plane in range(4)], (0, 0))
                for part in range(3):
                    total[part] = jnp.zeros((rows, tiles * LANES), jnp.float32)
            else:
                for part in range(3):
                    total[part] = total_in[part]
            load_windows(field, [(plane, plane) for plane in range(5)], (low_off, 1))
            for plane in range(5):
                field[plane, 0] = zero_column
                field[plane, tiles + 1] = zero_column

            for turn in range(ICE_DEPTH):
                stress_spans = spans(2 * turn + 1)
                speed_spans = spans(2 * turn + 2)

                def stress(group, column):
                    for span in stress_spans:
                        row = span + low_off
                        cache = {}
                        side_x = sides(field, 0, column, row, cache)
                        side_y = sides(field, 1, column, row, cache)
                        for i in range(GROUP):
                            here = column[i + 1]
                            left_x, right_x = side_x(i)
                            left_y, right_y = side_y(i)
                            row_x = (
                                field[0, here, pl.ds(row + 1, 8), :]
                                - field[0, here, pl.ds(row - 1, 8), :]
                            )
                            row_y = (
                                field[1, here, pl.ds(row + 1, 8), :]
                                - field[1, here, pl.ds(row - 1, 8), :]
                            )
                            col_x = right_x - left_x
                            col_y = right_y - left_y
                            strain_d = row_x + col_y
                            strain_t = row_x - col_y
                            strain_s = col_x + row_y
                            quarter_t = 0.25 * strain_t
                            square = (
                                strain_d * strain_d
                                + quarter_t * strain_t
                                + 0.25 * (strain_s * strain_s)
                                + 0.04
                            )
                            press = stat[0, column[i], pl.ds(span, 8), :]
                            scaled = press * lax.rsqrt(square)
                            at = (here, pl.ds(row, 8), slice(None))
                            field[(2,) + at] = keep * field[(2,) + at] + (
                                scaled * (strain_d + quarter_t) - press
                            )
                            field[(3,) + at] = keep * field[(3,) + at] + (
                                scaled * (strain_d - quarter_t) - press
                            )
                            field[(4,) + at] = keep * field[(4,) + at] + scaled * (
                                0.25 * strain_s
                            )

                def speed(group, column):
                    for span in speed_spans:
                        row = span + low_off
                        cache = {}
                        side_q = sides(field, 4, column, row, cache)
                        side_m = sides(field, 3, column, row, cache)
                        for i in range(GROUP):
                            here = column[i + 1]
                            left_q, right_q = side_q(i)
                            left_m, right_m = side_m(i)
                            force_x = (
                                field[2, here, pl.ds(row + 1, 8), :]
                                - field[2, here, pl.ds(row - 1, 8), :]
                            ) + (right_q - left_q)
                            force_y = (
                                field[4, here, pl.ds(row + 1, 8), :]
                                - field[4, here, pl.ds(row - 1, 8), :]
                            ) + (right_m - left_m)
                            at = (here, pl.ds(row, 8), slice(None))
                            old_x = field[(0,) + at]
                            old_y = field[(1,) + at]
                            beside = (column[i], pl.ds(span, 8), slice(None))
                            g = stat[(1,) + beside]
                            held = jnp.where(g > 0.0, 1.0 - g, 0.0)
                            quarter = 0.25 * g
                            field[(0,) + at] = (
                                held * (old_x + coriolis * old_y)
                                + quarter * force_x
                                + stat[(2,) + beside]
                            )
                            field[(1,) + at] = (
                                held * (old_y - coriolis * old_x)
                                + quarter * force_y
                                + stat[(3,) + beside]
                            )
                    for i in range(GROUP):
                        here = column[i + 1]
                        new_x = field[0, here, pl.ds(rows + low_off, 8), :]
                        new_y = field[1, here, pl.ds(rows + low_off, 8), :]
                        lanes = pl.ds(pl.multiple_of(column[i] * LANES, LANES), LANES)
                        total[0, :, lanes] += new_x
                        total[1, :, lanes] += new_y
                        total[2, :, lanes] += jnp.sqrt(1.0 + new_x * new_x + new_y * new_y)

                over_tiles(stress)
                over_tiles(speed)

            for c in range(tiles):
                lanes = slice(c * LANES, (c + 1) * LANES)
                mine = [field[p, c + 1, low_off + rows : low_off + 2 * rows, :] for p in range(5)]
                if last:
                    mine[2:] = [
                        0.5 * (mine[2] + mine[3]),
                        0.5 * (mine[2] - mine[3]),
                        0.5 * mine[4],
                    ]
                    covered = cover[:, lanes].astype(jnp.float32)
                    total[0, :, lanes] = (
                        total[0, :, lanes] * (1.0 / SUBCYCLES) - covered * current[0, :, lanes]
                    )
                    total[1, :, lanes] = (
                        total[1, :, lanes] * (1.0 / SUBCYCLES) - covered * current[1, :, lanes]
                    )
                    total[2, :, lanes] = (
                        total[2, :, lanes] * (melt[0, :, lanes] * covered) * (1.0 / SUBCYCLES)
                    )
                for p in range(5):
                    out[p, :, lanes] = mine[p]

        def ocean():
            if first:
                load_windows(stat, [(plane, 5 + plane) for plane in range(2)], (0, 0))
                for entry in range(2):
                    links[entry] = targets[entry].astype(jnp.float32)
                    links[2 + entry] = weights[entry].astype(jnp.float32)
            if not ocean_active:
                out[...] = own[:5]
                return
            load_windows(field, [(plane, plane) for plane in range(5)], (low_off, 1))
            for plane in range(5):
                for ref in (field, other):
                    ref[plane, 0] = zero_column
                    ref[plane, tiles + 1] = zero_column

            for turn in range(OCEAN_DEPTH):
                source, target = (field, other) if turn % 2 == 0 else (other, field)
                row_spans = spans(turn + 1)

                def advect(group, column):
                    for span in row_spans:
                        row = span + low_off
                        pos_x, neg_x, pos_y, neg_y = [], [], [], []
                        for i in range(GROUP):
                            beside = (column[i], pl.ds(span, 8), slice(None))
                            ux = courant * stat[(0,) + beside]
                            uy = courant * stat[(1,) + beside]
                            pos_x.append(jnp.maximum(ux, 0.0))
                            neg_x.append(jnp.minimum(ux, 0.0))
                            pos_y.append(jnp.maximum(uy, 0.0))
                            neg_y.append(jnp.minimum(uy, 0.0))
                        for level in range(5):
                            side = sides(source, level, column, row, {})
                            for i in range(GROUP):
                                here = column[i + 1]
                                left, right = side(i)
                                centre = source[level, here, pl.ds(row, 8), :]
                                below = source[level, here, pl.ds(row - 1, 8), :]
                                above = source[level, here, pl.ds(row + 1, 8), :]
                                change = (
                                    pos_x[i] * (centre - below)
                                    + neg_x[i] * (above - centre)
                                    + pos_y[i] * (centre - left)
                                    + neg_y[i] * (right - centre)
                                )
                                if level:
                                    change = level_speed[level] * change
                                target[level, here, pl.ds(row, 8), :] = centre - change

                over_tiles(advect)

            done = field if OCEAN_DEPTH % 2 == 0 else other
            for p in range(5):
                for c in range(tiles):
                    out[p, :, c * LANES : (c + 1) * LANES] = done[
                        p, c + 1, low_off + rows : low_off + 2 * rows, :
                    ]

        @pl.when(flag[0] < strips)
        def _():
            ice()

        @pl.when(flag[0] >= strips)
        def _():
            ocean()

    return kernel


WIDE = 256


def scatter_half(half, values, spots_of, weights_of, sums, blocks):
    rows = values.shape[1]
    columns = values.shape[2]
    groups = columns // WIDE
    spots = rows * groups
    turns = 2 * rows
    sums[...] = jnp.zeros_like(sums)
    high_at = lax.broadcasted_iota(jnp.int32, (spots, columns), 0).astype(jnp.bfloat16)
    low_at = lax.broadcasted_iota(jnp.int32, (WIDE, columns), 0).astype(jnp.bfloat16)
    zero = jnp.zeros((), jnp.bfloat16)
    one = jnp.ones((), jnp.bfloat16)

    def build(turn, left, right):
        entry = turn // rows
        row = turn % rows
        spot = spots_of[entry, pl.ds(row, 1), :].astype(jnp.int32)
        scale = weights_of[entry, pl.ds(row, 1), :].astype(jnp.float32) / weight_norm
        low = jnp.bitwise_and(spot, WIDE - 1)
        high = jnp.right_shift(spot, 8) - half * spots
        inside = jnp.logical_and(high >= 0, high < spots)
        place = jnp.bitwise_and(high, groups - 1) * rows + high // groups
        place = jnp.where(inside, place, -1)
        low = low.astype(jnp.float32).astype(jnp.bfloat16)
        place = place.astype(jnp.float32).astype(jnp.bfloat16)
        right[...] = jnp.where(low_at == low, one, zero)
        hit = high_at == place
        for channel in range(3):
            value = values[channel, pl.ds(row, 1), :] * scale
            coarse = value.astype(jnp.bfloat16)
            fine = (value - coarse.astype(jnp.float32)).astype(jnp.bfloat16)
            for part, piece in enumerate((coarse, fine)):
                first = (2 * channel + part) * spots
                left[first : first + spots, :] = jnp.where(hit, piece, zero)

    def multiply(left, right):
        sums[...] += lax.dot_general(
            left[...],
            right[...],
            (((1,), (1,)), ((), ())),
            preferred_element_type=jnp.float32,
        )

    left_a, right_a, left_b, right_b = blocks
    build(0, left_a, right_a)

    def step(pair, carry):
        build(2 * pair + 1, left_b, right_b)
        multiply(left_a, right_a)
        build(jnp.minimum(2 * pair + 2, turns - 1), left_a, right_a)
        multiply(left_b, right_b)
        return carry

    lax.fori_loop(0, turns // 2, step, 0)

    def tile(channel, group):
        first = 2 * channel * spots + group * rows
        return sums[first : first + rows, :] + sums[first + spots : first + spots + rows, :]

    return tile, groups


def write_half(half, values, spots_of, weights_of, out, sums, blocks):
    tile, groups = scatter_half(half, values, spots_of, weights_of, sums, blocks)
    for channel in range(3):
        for g in range(groups):
            out[channel, :, g * WIDE : (g + 1) * WIDE] = tile(channel, g)


def lower_kernel(strips, flag, average, targets, weights, out, sums, *blocks):
    @pl.when(flag[0] < strips)
    def _():
        write_half(0, average, targets, weights, out, sums, blocks)


def upper_kernel(strips, flag, before, links, out, sums, *blocks):
    @pl.when(flag[0] >= strips)
    def _():
        write_half(1, before, links.at[:2], links.at[2:], out, sums, blocks)


def final_kernel(strips, flag, fields, average, lower, upper, state, coupled):
    @pl.when(flag[0] < strips)
    def _():
        state[0] = fields[...]
        coupled[0] = average[...]

    @pl.when(flag[0] >= strips)
    def _():
        flux = lower[...] + upper[...]
        coupled[0] = flux
        state[0, 0] = fields[0] - dilution * flux[2]
        state[0, 1:] = fields[1:]


def body(initial, ice_forcing, ocean_current, ice_cover, targets, weights):
    rows, columns = initial.shape[2:]
    tiles = columns // LANES
    strips = lax.axis_size("blk")
    both = ("comp", "blk")
    flag = lax.axis_index(both).astype(jnp.int32).reshape(1)

    def swapped(value, kinds, start):
        pairs = [
            (kind * strips + source, kind * strips + target)
            for kind in kinds
            for b in range(start, strips - 1, 2)
            for source, target in ((b, b + 1), (b + 1, b))
        ]
        return lax.ppermute(value, both, pairs)

    def shape(*dims):
        return pltpu.VMEM(dims, jnp.float32)

    def held(*values):
        return [pltpu.with_memory_space_constraint(value, pltpu.VMEM) for value in values]

    block = pl.pallas_call(
        partial(prep_kernel, strips),
        compiler_params=LIMITED,
        out_shape=shape(9, rows, columns),
        in_specs=[SMEM] + [pl.BlockSpec(memory_space=pltpu.HBM)] * 4,
        out_specs=VMEM,
        scratch_shapes=[
            pltpu.VMEM(value.shape, value.dtype)
            for value in (initial, ice_forcing, ocean_current, ice_cover)
        ]
        + [pltpu.SemaphoreType.DMA((4,))],
    )(
        flag,
        *(
            pltpu.with_memory_space_constraint(value, pltpu.HBM)
            for value in (initial, ice_forcing, ocean_current, ice_cover)
        ),
    )

    rounds = SUBCYCLES // ICE_DEPTH
    each = OCEAN_DEPTH // ICE_DEPTH
    window = 3 * rows
    stat = total = None
    for turn in range(rounds):
        first, last = turn == 0, turn == rounds - 1
        active = turn % each == 0
        kinds = (0, 1) if active else (0,)
        near = swapped(block, kinds, 0)
        far = swapped(block, kinds, 1)
        operands = [flag, block, near, far]
        outs = [shape(5, rows, columns), shape(3, rows, columns)]
        operands += [targets, weights] if first else [stat, total]
        if last:
            operands += [ice_forcing[4:], ocean_current, ice_cover]
        if first:
            outs += [shape(4, tiles, window, LANES), shape(4, rows, columns)]
        done = pl.pallas_call(
            make_round(strips, first, last, active, rows, tiles),
            compiler_params=LIMITED,
            out_shape=outs,
            in_specs=[SMEM] + [VMEM] * (len(operands) - 1),
            out_specs=[VMEM] * len(outs),
            scratch_shapes=[pltpu.VMEM((5, tiles + 2, window + 2 * PAD, LANES), jnp.float32)] * 2,
        )(flag, *held(*operands[1:]))
        block, total = done[:2]
        if first:
            stat, links = done[2:]

    average = total
    links_before = lax.ppermute(
        links, both, [(strips + b, strips + (b + 1) % strips) for b in range(strips)]
    )
    before = lax.ppermute(average, both, [(b, strips + (b + 1) % strips) for b in range(strips)])
    spots = rows * columns // WIDE
    scratch = [pltpu.VMEM((6 * spots, WIDE), jnp.float32)] + [
        pltpu.VMEM((6 * spots, columns), jnp.bfloat16),
        pltpu.VMEM((WIDE, columns), jnp.bfloat16),
    ] * 2

    def scattered(kernel, *operands):
        return pl.pallas_call(
            partial(kernel, strips),
            compiler_params=LIMITED,
            out_shape=shape(3, rows, columns),
            in_specs=[SMEM] + [VMEM] * len(operands),
            out_specs=VMEM,
            scratch_shapes=scratch,
        )(flag, *held(*operands))

    lower = scattered(lower_kernel, average, targets, weights)
    received = lax.ppermute(lower, both, [(b, strips + b) for b in range(strips)])
    upper = scattered(upper_kernel, before, links_before)
    return tuple(
        pl.pallas_call(
            partial(final_kernel, strips),
            compiler_params=LIMITED,
            out_shape=[
                jax.ShapeDtypeStruct((1, 5, rows, columns), jnp.float32),
                jax.ShapeDtypeStruct((1, 3, rows, columns), jnp.float32),
            ],
            in_specs=[SMEM] + [VMEM] * 4,
            out_specs=[VMEM] * 2,
        )(flag, *held(block, average, received, upper))
    )


def solution(mesh):
    placed = (
        P("comp", None, "blk", None),
        P(None, "blk", None),
        P(None, "blk", None),
        P("blk", None),
        P(None, "blk", None),
        P(None, "blk", None),
    )
    return jax.shard_map(
        body,
        mesh=mesh,
        in_specs=placed,
        out_specs=(P("comp", None, "blk", None), P("comp", None, "blk", None)),
        check_vma=False,
    )
```

```python
from functools import partial

import jax
import jax.numpy as jnp
from jax import lax
from jax.experimental import pallas as pl
from jax.experimental.pallas import tpu as pltpu
from jax.sharding import PartitionSpec as P

SUBCYCLES = 16
ICE_DEPTH = 4
OCEAN_DEPTH = 8
LANES = 128
PAD = 8
GROUP = 16
OCEAN_DELAY = 12000

keep = 1.0 / 1.5
gain = 0.5 / 1.5
coriolis = 0.1
drag_coef = 1.0
inertia = 4.0
courant = 0.2
dilution = 0.5
weight_norm = 4.0
level_speed = (1.0, 0.8, 0.6, 0.45, 0.3)

VMEM = pl.BlockSpec(memory_space=pltpu.VMEM)
SMEM = pl.BlockSpec(memory_space=pltpu.SMEM)
LIMITED = pltpu.CompilerParams(vmem_limit_bytes=20 * 1024 * 1024)


def prep_kernel(strips, flag, *refs):
    sources, out, (initial, forcing, current, cover), arrived = refs[:4], refs[4], refs[5:9], refs[9]
    copies = [
        pltpu.make_async_copy(source, target, arrived.at[i])
        for i, (source, target) in enumerate(zip(sources, (initial, forcing, current, cover)))
    ]
    for copy in copies:
        copy.start()
    for copy in copies:
        copy.wait()

    @pl.when(flag[0] < strips)
    def _():
        out[0] = initial[0, 0]
        out[1] = initial[0, 1]
        out[2] = initial[0, 2] + initial[0, 3]
        out[3] = initial[0, 2] - initial[0, 3]
        out[4] = 2.0 * initial[0, 4]
        covered = cover[...].astype(jnp.float32)
        out[5] = gain * forcing[1] * covered
        g = covered / (inertia * forcing[0] + drag_coef)
        out[6] = g
        out[7] = g * (forcing[2] + drag_coef * current[0])
        out[8] = g * (forcing[3] + drag_coef * current[1])

    @pl.when(flag[0] >= strips)
    def _():
        pl.delay(OCEAN_DELAY)
        for level in range(5):
            out[level] = initial[0, level]
        out[5] = current[0]
        out[6] = current[1]
        out[7] = jnp.zeros_like(current[0])
        out[8] = jnp.zeros_like(current[0])


def load_strip(dst, dst_plane, src, src_plane, part, tiles, base):
    rows = src.shape[1]
    for c in range(tiles):
        dst[dst_plane, base[1] + c, pl.ds(base[0] + part * rows, rows), :] = src[
            src_plane, :, c * LANES : (c + 1) * LANES
        ]


def make_round(strips, first, last, ocean_active, rows, tiles):
    window = 3 * rows
    low_off = PAD

    def spans(margin):
        count = window - 2 * margin
        if count <= 8:
            return (8,)
        if count <= 16:
            return (4, 12)
        return (0, 8, 16)

    def kernel(*refs):
        refs = list(refs)
        flag = refs.pop(0)
        own, far, near = refs[:3]
        refs = refs[3:]
        if first:
            targets, weights = refs[:2]
        else:
            stat, total_in = refs[:2]
        refs = refs[2:]
        if last:
            melt, current, cover = refs[:3]
            refs = refs[3:]
        if first:
            out, total, stat, links = refs[:4]
            refs = refs[4:]
        else:
            out, total = refs[:2]
            refs = refs[2:]
        field, other = refs

        lane = lax.broadcasted_iota(jnp.int32, (8, LANES), 1)
        at_first = lane == 0
        at_last = lane == LANES - 1
        odd = jnp.bitwise_and(flag[0], 1) == 1

        def load_windows(dst, planes, base):
            def halo(low, high):
                for plane, source in planes:
                    load_strip(dst, plane, low, source, 0, tiles, base)
                    load_strip(dst, plane, high, source, 2, tiles, base)

            for plane, source in planes:
                load_strip(dst, plane, own, source, 1, tiles, base)
            pl.when(odd)(lambda: halo(near, far))
            pl.when(jnp.logical_not(odd))(lambda: halo(far, near))

        zero_column = jnp.zeros((window + 2 * PAD, LANES), jnp.float32)

        def sides(ref, plane, column, row, cache):
            def rolled(c, shift):
                key = (plane, c, row, shift)
                if key not in cache:
                    tile = ref[plane, column[c], pl.ds(row, 8), :]
                    cache[key] = pltpu.roll(tile, shift, 1)
                return cache[key]

            def at(i):
                left = jnp.where(at_first, rolled(i, 1), rolled(i + 1, 1))
                right = jnp.where(at_last, rolled(i + 2, LANES - 1), rolled(i + 1, LANES - 1))
                return left, right

            return at

        def over_tiles(body):
            def step(group, carry):
                column = [group * GROUP + i for i in range(GROUP + 2)]
                body(group, column)
                return carry

            lax.fori_loop(0, tiles // GROUP, step, 0)

        def ice():
            if first:
                load_windows(stat, [(plane, 5 + plane) for plane in range(4)], (0, 0))
                for part in range(3):
                    total[part] = jnp.zeros((rows, tiles * LANES), jnp.float32)
            else:
                for part in range(3):
                    total[part] = total_in[part]
            load_windows(field, [(plane, plane) for plane in range(5)], (low_off, 1))
            for plane in range(5):
                field[plane, 0] = zero_column
                field[plane, tiles + 1] = zero_column

            for turn in range(ICE_DEPTH):
                stress_spans = spans(2 * turn + 1)
                speed_spans = spans(2 * turn + 2)

                def stress(group, column):
                    for span in stress_spans:
                        row = span + low_off
                        cache = {}
                        side_x = sides(field, 0, column, row, cache)
                        side_y = sides(field, 1, column, row, cache)
                        for i in range(GROUP):
                            here = column[i + 1]
                            left_x, right_x = side_x(i)
                            left_y, right_y = side_y(i)
                            row_x = (
                                field[0, here, pl.ds(row + 1, 8), :]
                                - field[0, here, pl.ds(row - 1, 8), :]
                            )
                            row_y = (
                                field[1, here, pl.ds(row + 1, 8), :]
                                - field[1, here, pl.ds(row - 1, 8), :]
                            )
                            col_x = right_x - left_x
                            col_y = right_y - left_y
                            strain_d = row_x + col_y
                            strain_t = row_x - col_y
                            strain_s = col_x + row_y
                            quarter_t = 0.25 * strain_t
                            square = (
                                strain_d * strain_d
                                + quarter_t * strain_t
                                + 0.25 * (strain_s * strain_s)
                                + 0.04
                            )
                            press = stat[0, column[i], pl.ds(span, 8), :]
                            scaled = press * lax.rsqrt(square)
                            at = (here, pl.ds(row, 8), slice(None))
                            field[(2,) + at] = keep * field[(2,) + at] + (
                                scaled * (strain_d + quarter_t) - press
                            )
                            field[(3,) + at] = keep * field[(3,) + at] + (
                                scaled * (strain_d - quarter_t) - press
                            )
                            field[(4,) + at] = keep * field[(4,) + at] + scaled * (
                                0.25 * strain_s
                            )

                def speed(group, column):
                    for span in speed_spans:
                        row = span + low_off
                        cache = {}
                        side_q = sides(field, 4, column, row, cache)
                        side_m = sides(field, 3, column, row, cache)
                        for i in range(GROUP):
                            here = column[i + 1]
                            left_q, right_q = side_q(i)
                            left_m, right_m = side_m(i)
                            force_x = (
                                field[2, here, pl.ds(row + 1, 8), :]
                                - field[2, here, pl.ds(row - 1, 8), :]
                            ) + (right_q - left_q)
                            force_y = (
                                field[4, here, pl.ds(row + 1, 8), :]
                                - field[4, here, pl.ds(row - 1, 8), :]
                            ) + (right_m - left_m)
                            at = (here, pl.ds(row, 8), slice(None))
                            old_x = field[(0,) + at]
                            old_y = field[(1,) + at]
                            beside = (column[i], pl.ds(span, 8), slice(None))
                            g = stat[(1,) + beside]
                            held = jnp.where(g > 0.0, 1.0 - g, 0.0)
                            quarter = 0.25 * g
                            field[(0,) + at] = (
                                held * (old_x + coriolis * old_y)
                                + quarter * force_x
                                + stat[(2,) + beside]
                            )
                            field[(1,) + at] = (
                                held * (old_y - coriolis * old_x)
                                + quarter * force_y
                                + stat[(3,) + beside]
                            )
                    for i in range(GROUP):
                        here = column[i + 1]
                        new_x = field[0, here, pl.ds(rows + low_off, 8), :]
                        new_y = field[1, here, pl.ds(rows + low_off, 8), :]
                        lanes = pl.ds(pl.multiple_of(column[i] * LANES, LANES), LANES)
                        total[0, :, lanes] += new_x
                        total[1, :, lanes] += new_y
                        total[2, :, lanes] += jnp.sqrt(1.0 + new_x * new_x + new_y * new_y)

                over_tiles(stress)
                over_tiles(speed)

            for c in range(tiles):
                lanes = slice(c * LANES, (c + 1) * LANES)
                mine = [field[p, c + 1, low_off + rows : low_off + 2 * rows, :] for p in range(5)]
                if last:
                    mine[2:] = [
                        0.5 * (mine[2] + mine[3]),
                        0.5 * (mine[2] - mine[3]),
                        0.5 * mine[4],
                    ]
                    covered = cover[:, lanes].astype(jnp.float32)
                    total[0, :, lanes] = (
                        total[0, :, lanes] * (1.0 / SUBCYCLES) - covered * current[0, :, lanes]
                    )
                    total[1, :, lanes] = (
                        total[1, :, lanes] * (1.0 / SUBCYCLES) - covered * current[1, :, lanes]
                    )
                    total[2, :, lanes] = (
                        total[2, :, lanes] * (melt[0, :, lanes] * covered) * (1.0 / SUBCYCLES)
                    )
                for p in range(5):
                    out[p, :, lanes] = mine[p]

        def ocean():
            if first:
                load_windows(stat, [(plane, 5 + plane) for plane in range(2)], (0, 0))
                for entry in range(2):
                    links[entry] = targets[entry].astype(jnp.float32)
                    links[2 + entry] = weights[entry].astype(jnp.float32)
            if not ocean_active:
                out[...] = own[:5]
                return
            load_windows(field, [(plane, plane) for plane in range(5)], (low_off, 1))
            for plane in range(5):
                for ref in (field, other):
                    ref[plane, 0] = zero_column
                    ref[plane, tiles + 1] = zero_column

            for turn in range(OCEAN_DEPTH):
                source, target = (field, other) if turn % 2 == 0 else (other, field)
                row_spans = spans(turn + 1)

                def advect(group, column):
                    for span in row_spans:
                        row = span + low_off
                        pos_x, neg_x, pos_y, neg_y = [], [], [], []
                        for i in range(GROUP):
                            beside = (column[i], pl.ds(span, 8), slice(None))
                            ux = courant * stat[(0,) + beside]
                            uy = courant * stat[(1,) + beside]
                            pos_x.append(jnp.maximum(ux, 0.0))
                            neg_x.append(jnp.minimum(ux, 0.0))
                            pos_y.append(jnp.maximum(uy, 0.0))
                            neg_y.append(jnp.minimum(uy, 0.0))
                        for level in range(5):
                            side = sides(source, level, column, row, {})
                            for i in range(GROUP):
                                here = column[i + 1]
                                left, right = side(i)
                                centre = source[level, here, pl.ds(row, 8), :]
                                below = source[level, here, pl.ds(row - 1, 8), :]
                                above = source[level, here, pl.ds(row + 1, 8), :]
                                change = (
                                    pos_x[i] * (centre - below)
                                    + neg_x[i] * (above - centre)
                                    + pos_y[i] * (centre - left)
                                    + neg_y[i] * (right - centre)
                                )
                                if level:
                                    change = level_speed[level] * change
                                target[level, here, pl.ds(row, 8), :] = centre - change

                over_tiles(advect)

            done = field if OCEAN_DEPTH % 2 == 0 else other
            for p in range(5):
                for c in range(tiles):
                    out[p, :, c * LANES : (c + 1) * LANES] = done[
                        p, c + 1, low_off + rows : low_off + 2 * rows, :
                    ]

        @pl.when(flag[0] < strips)
        def _():
            ice()

        @pl.when(flag[0] >= strips)
        def _():
            ocean()

    return kernel


WIDE = 256


def scatter_half(half, values, spots_of, weights_of, sums, blocks):
    rows = values.shape[1]
    columns = values.shape[2]
    groups = columns // WIDE
    spots = rows * groups
    turns = 2 * rows
    sums[...] = jnp.zeros_like(sums)
    high_at = lax.broadcasted_iota(jnp.int32, (spots, columns), 0).astype(jnp.bfloat16)
    low_at = lax.broadcasted_iota(jnp.int32, (WIDE, columns), 0).astype(jnp.bfloat16)
    zero = jnp.zeros((), jnp.bfloat16)
    one = jnp.ones((), jnp.bfloat16)

    def build(turn, left, right):
        entry = turn // rows
        row = turn % rows
        spot = spots_of[entry, pl.ds(row, 1), :].astype(jnp.int32)
        scale = weights_of[entry, pl.ds(row, 1), :].astype(jnp.float32) / weight_norm
        low = jnp.bitwise_and(spot, WIDE - 1)
        high = jnp.right_shift(spot, 8) - half * spots
        inside = jnp.logical_and(high >= 0, high < spots)
        place = jnp.bitwise_and(high, groups - 1) * rows + high // groups
        place = jnp.where(inside, place, -1)
        low = low.astype(jnp.float32).astype(jnp.bfloat16)
        place = place.astype(jnp.float32).astype(jnp.bfloat16)
        right[...] = jnp.where(low_at == low, one, zero)
        hit = high_at == place
        for channel in range(3):
            value = values[channel, pl.ds(row, 1), :] * scale
            coarse = value.astype(jnp.bfloat16)
            fine = (value - coarse.astype(jnp.float32)).astype(jnp.bfloat16)
            for part, piece in enumerate((coarse, fine)):
                first = (2 * channel + part) * spots
                left[first : first + spots, :] = jnp.where(hit, piece, zero)

    def multiply(left, right):
        sums[...] += lax.dot_general(
            left[...],
            right[...],
            (((1,), (1,)), ((), ())),
            preferred_element_type=jnp.float32,
        )

    left_a, right_a, left_b, right_b = blocks
    build(0, left_a, right_a)

    def step(pair, carry):
        build(2 * pair + 1, left_b, right_b)
        multiply(left_a, right_a)
        build(jnp.minimum(2 * pair + 2, turns - 1), left_a, right_a)
        multiply(left_b, right_b)
        return carry

    lax.fori_loop(0, turns // 2, step, 0)

    def tile(channel, group):
        first = 2 * channel * spots + group * rows
        return sums[first : first + rows, :] + sums[first + spots : first + spots + rows, :]

    return tile, groups


def write_half(half, values, spots_of, weights_of, out, sums, blocks):
    tile, groups = scatter_half(half, values, spots_of, weights_of, sums, blocks)
    for channel in range(3):
        for g in range(groups):
            out[channel, :, g * WIDE : (g + 1) * WIDE] = tile(channel, g)


def lower_kernel(strips, flag, average, targets, weights, out, sums, *blocks):
    @pl.when(flag[0] < strips)
    def _():
        write_half(0, average, targets, weights, out, sums, blocks)


def upper_kernel(strips, flag, before, links, out, sums, *blocks):
    @pl.when(flag[0] >= strips)
    def _():
        write_half(1, before, links.at[:2], links.at[2:], out, sums, blocks)


def final_kernel(strips, flag, fields, average, lower, upper, state, coupled):
    @pl.when(flag[0] < strips)
    def _():
        state[0] = fields[...]
        coupled[0] = average[...]

    @pl.when(flag[0] >= strips)
    def _():
        flux = lower[...] + upper[...]
        coupled[0] = flux
        state[0, 0] = fields[0] - dilution * flux[2]
        state[0, 1:] = fields[1:]


def body(initial, ice_forcing, ocean_current, ice_cover, targets, weights):
    rows, columns = initial.shape[2:]
    tiles = columns // LANES
    strips = lax.axis_size("blk")
    both = ("comp", "blk")
    flag = lax.axis_index(both).astype(jnp.int32).reshape(1)

    def swapped(value, kinds, start):
        pairs = [
            (kind * strips + source, kind * strips + target)
            for kind in kinds
            for b in range(start, strips - 1, 2)
            for source, target in ((b, b + 1), (b + 1, b))
        ]
        return lax.ppermute(value, both, pairs)

    def shape(*dims):
        return pltpu.VMEM(dims, jnp.float32)

    def held(*values):
        return [pltpu.with_memory_space_constraint(value, pltpu.VMEM) for value in values]

    block = pl.pallas_call(
        partial(prep_kernel, strips),
        compiler_params=LIMITED,
        out_shape=shape(9, rows, columns),
        in_specs=[SMEM] + [pl.BlockSpec(memory_space=pltpu.HBM)] * 4,
        out_specs=VMEM,
        scratch_shapes=[
            pltpu.VMEM(value.shape, value.dtype)
            for value in (initial, ice_forcing, ocean_current, ice_cover)
        ]
        + [pltpu.SemaphoreType.DMA((4,))],
    )(
        flag,
        *(
            pltpu.with_memory_space_constraint(value, pltpu.HBM)
            for value in (initial, ice_forcing, ocean_current, ice_cover)
        ),
    )

    rounds = SUBCYCLES // ICE_DEPTH
    each = OCEAN_DEPTH // ICE_DEPTH
    window = 3 * rows
    stat = total = None
    for turn in range(rounds):
        first, last = turn == 0, turn == rounds - 1
        active = turn % each == 0
        kinds = (0, 1) if active else (0,)
        near = swapped(block, kinds, 0)
        far = swapped(block, kinds, 1)
        operands = [flag, block, far, near]
        outs = [shape(5, rows, columns), shape(3, rows, columns)]
        operands += [targets, weights] if first else [stat, total]
        if last:
            operands += [ice_forcing[4:], ocean_current, ice_cover]
        if first:
            outs += [shape(4, tiles, window, LANES), shape(4, rows, columns)]
        done = pl.pallas_call(
            make_round(strips, first, last, active, rows, tiles),
            compiler_params=LIMITED,
            out_shape=outs,
            in_specs=[SMEM] + [VMEM] * (len(operands) - 1),
            out_specs=[VMEM] * len(outs),
            scratch_shapes=[pltpu.VMEM((5, tiles + 2, window + 2 * PAD, LANES), jnp.float32)] * 2,
        )(flag, *held(*operands[1:]))
        block, total = done[:2]
        if first:
            stat, links = done[2:]

    average = total
    links_before = lax.ppermute(
        links, both, [(strips + b, strips + (b + 1) % strips) for b in range(strips)]
    )
    before = lax.ppermute(average, both, [(b, strips + (b + 1) % strips) for b in range(strips)])
    spots = rows * columns // WIDE
    scratch = [pltpu.VMEM((6 * spots, WIDE), jnp.float32)] + [
        pltpu.VMEM((6 * spots, columns), jnp.bfloat16),
        pltpu.VMEM((WIDE, columns), jnp.bfloat16),
    ] * 2

    def scattered(kernel, *operands):
        return pl.pallas_call(
            partial(kernel, strips),
            compiler_params=LIMITED,
            out_shape=shape(3, rows, columns),
            in_specs=[SMEM] + [VMEM] * len(operands),
            out_specs=VMEM,
            scratch_shapes=scratch,
        )(flag, *held(*operands))

    lower = scattered(lower_kernel, average, targets, weights)
    received = lax.ppermute(lower, both, [(b, strips + b) for b in range(strips)])
    upper = scattered(upper_kernel, before, links_before)
    return tuple(
        pl.pallas_call(
            partial(final_kernel, strips),
            compiler_params=LIMITED,
            out_shape=[
                jax.ShapeDtypeStruct((1, 5, rows, columns), jnp.float32),
                jax.ShapeDtypeStruct((1, 3, rows, columns), jnp.float32),
            ],
            in_specs=[SMEM] + [VMEM] * 4,
            out_specs=[VMEM] * 2,
        )(flag, *held(block, average, received, upper))
    )


def solution(mesh):
    placed = (
        P("comp", None, "blk", None),
        P(None, "blk", None),
        P(None, "blk", None),
        P("blk", None),
        P(None, "blk", None),
        P(None, "blk", None),
    )
    return jax.shard_map(
        body,
        mesh=mesh,
        in_specs=placed,
        out_specs=(P("comp", None, "blk", None), P("comp", None, "blk", None)),
        check_vma=False,
    )
```

```python
from functools import partial

import jax
import jax.numpy as jnp
from jax import lax
from jax.experimental import pallas as pl
from jax.experimental.pallas import tpu as pltpu
from jax.sharding import PartitionSpec as P

SUBCYCLES = 16
ICE_DEPTH = 4
OCEAN_DEPTH = 8
LANES = 128
PAD = 8
GROUP = 16
OCEAN_DELAY = 12000

keep = 1.0 / 1.5
gain = 0.5 / 1.5
coriolis = 0.1
drag_coef = 1.0
inertia = 4.0
courant = 0.2
dilution = 0.5
weight_norm = 4.0
level_speed = (1.0, 0.8, 0.6, 0.45, 0.3)

VMEM = pl.BlockSpec(memory_space=pltpu.VMEM)
SMEM = pl.BlockSpec(memory_space=pltpu.SMEM)
LIMITED = pltpu.CompilerParams(vmem_limit_bytes=20 * 1024 * 1024)


def prep_kernel(strips, flag, *refs):
    sources, (out, extra), landed, arrived = refs[:6], refs[6:8], refs[8:14], refs[14]
    initial, forcing, current, cover, targets, weights = landed
    copies = [
        pltpu.make_async_copy(source, target, arrived.at[i])
        for i, (source, target) in enumerate(zip(sources, landed))
    ]
    for copy in copies:
        copy.start()
    for copy in copies:
        copy.wait()

    @pl.when(flag[0] < strips)
    def _():
        out[0] = initial[0, 0]
        out[1] = initial[0, 1]
        out[2] = initial[0, 2] + initial[0, 3]
        out[3] = initial[0, 2] - initial[0, 3]
        out[4] = 2.0 * initial[0, 4]
        covered = cover[...].astype(jnp.float32)
        out[5] = gain * forcing[1] * covered
        g = covered / (inertia * forcing[0] + drag_coef)
        out[6] = g
        out[7] = g * (forcing[2] + drag_coef * current[0])
        out[8] = g * (forcing[3] + drag_coef * current[1])
        extra[0] = covered * current[0]
        extra[1] = covered * current[1]
        extra[2] = covered * forcing[4]

    @pl.when(flag[0] >= strips)
    def _():
        pl.delay(OCEAN_DELAY)
        for level in range(5):
            out[level] = initial[0, level]
        out[5] = current[0]
        out[6] = current[1]
        out[7] = jnp.zeros_like(current[0])
        out[8] = jnp.zeros_like(current[0])
        for entry in range(2):
            extra[entry] = targets[entry].astype(jnp.float32)
            extra[2 + entry] = weights[entry].astype(jnp.float32)


def load_strip(dst, dst_plane, src, src_plane, part, tiles, base):
    rows = src.shape[1]
    for c in range(tiles):
        dst[dst_plane, base[1] + c, pl.ds(base[0] + part * rows, rows), :] = src[
            src_plane, :, c * LANES : (c + 1) * LANES
        ]


def make_round(strips, first, last, ocean_active, rows, tiles):
    window = 3 * rows
    low_off = PAD

    def spans(margin):
        count = window - 2 * margin
        if count <= 8:
            return (8,)
        if count <= 16:
            return (4, 12)
        return (0, 8, 16)

    def kernel(*refs):
        refs = list(refs)
        flag = refs.pop(0)
        own, far, near = refs[:3]
        refs = refs[3:]
        if not first:
            stat, total_in = refs[:2]
            refs = refs[2:]
        if last:
            extra = refs.pop(0)
        if first:
            out, total, stat = refs[:3]
            refs = refs[3:]
        else:
            out, total = refs[:2]
            refs = refs[2:]
        field, other = refs

        lane = lax.broadcasted_iota(jnp.int32, (8, LANES), 1)
        at_first = lane == 0
        at_last = lane == LANES - 1
        odd = jnp.bitwise_and(flag[0], 1) == 1

        def load_windows(dst, planes, base):
            def halo(low, high):
                for plane, source in planes:
                    load_strip(dst, plane, low, source, 0, tiles, base)
                    load_strip(dst, plane, high, source, 2, tiles, base)

            for plane, source in planes:
                load_strip(dst, plane, own, source, 1, tiles, base)
            pl.when(odd)(lambda: halo(near, far))
            pl.when(jnp.logical_not(odd))(lambda: halo(far, near))

        zero_column = jnp.zeros((window + 2 * PAD, LANES), jnp.float32)

        def sides(ref, plane, column, row, cache):
            def rolled(c, shift):
                key = (plane, c, row, shift)
                if key not in cache:
                    tile = ref[plane, column[c], pl.ds(row, 8), :]
                    cache[key] = pltpu.roll(tile, shift, 1)
                return cache[key]

            def at(i):
                left = jnp.where(at_first, rolled(i, 1), rolled(i + 1, 1))
                right = jnp.where(at_last, rolled(i + 2, LANES - 1), rolled(i + 1, LANES - 1))
                return left, right

            return at

        def over_tiles(body):
            def step(group, carry):
                column = [group * GROUP + i for i in range(GROUP + 2)]
                body(group, column)
                return carry

            lax.fori_loop(0, tiles // GROUP, step, 0)

        def ice():
            if first:
                load_windows(stat, [(plane, 5 + plane) for plane in range(4)], (0, 0))
                for part in range(3):
                    total[part] = jnp.zeros((rows, tiles * LANES), jnp.float32)
            else:
                for part in range(3):
                    total[part] = total_in[part]
            load_windows(field, [(plane, plane) for plane in range(5)], (low_off, 1))
            for plane in range(5):
                field[plane, 0] = zero_column
                field[plane, tiles + 1] = zero_column

            for turn in range(ICE_DEPTH):
                stress_spans = spans(2 * turn + 1)
                speed_spans = spans(2 * turn + 2)

                def stress(group, column):
                    for span in stress_spans:
                        row = span + low_off
                        cache = {}
                        side_x = sides(field, 0, column, row, cache)
                        side_y = sides(field, 1, column, row, cache)
                        for i in range(GROUP):
                            here = column[i + 1]
                            left_x, right_x = side_x(i)
                            left_y, right_y = side_y(i)
                            row_x = (
                                field[0, here, pl.ds(row + 1, 8), :]
                                - field[0, here, pl.ds(row - 1, 8), :]
                            )
                            row_y = (
                                field[1, here, pl.ds(row + 1, 8), :]
                                - field[1, here, pl.ds(row - 1, 8), :]
                            )
                            col_x = right_x - left_x
                            col_y = right_y - left_y
                            strain_d = row_x + col_y
                            strain_t = row_x - col_y
                            strain_s = col_x + row_y
                            quarter_t = 0.25 * strain_t
                            square = (
                                strain_d * strain_d
                                + quarter_t * strain_t
                                + 0.25 * (strain_s * strain_s)
                                + 0.04
                            )
                            press = stat[0, column[i], pl.ds(span, 8), :]
                            scaled = press * lax.rsqrt(square)
                            at = (here, pl.ds(row, 8), slice(None))
                            field[(2,) + at] = keep * field[(2,) + at] + (
                                scaled * (strain_d + quarter_t) - press
                            )
                            field[(3,) + at] = keep * field[(3,) + at] + (
                                scaled * (strain_d - quarter_t) - press
                            )
                            field[(4,) + at] = keep * field[(4,) + at] + scaled * (
                                0.25 * strain_s
                            )

                def speed(group, column):
                    for span in speed_spans:
                        row = span + low_off
                        cache = {}
                        side_q = sides(field, 4, column, row, cache)
                        side_m = sides(field, 3, column, row, cache)
                        for i in range(GROUP):
                            here = column[i + 1]
                            left_q, right_q = side_q(i)
                            left_m, right_m = side_m(i)
                            force_x = (
                                field[2, here, pl.ds(row + 1, 8), :]
                                - field[2, here, pl.ds(row - 1, 8), :]
                            ) + (right_q - left_q)
                            force_y = (
                                field[4, here, pl.ds(row + 1, 8), :]
                                - field[4, here, pl.ds(row - 1, 8), :]
                            ) + (right_m - left_m)
                            at = (here, pl.ds(row, 8), slice(None))
                            old_x = field[(0,) + at]
                            old_y = field[(1,) + at]
                            beside = (column[i], pl.ds(span, 8), slice(None))
                            g = stat[(1,) + beside]
                            held = jnp.where(g > 0.0, 1.0 - g, 0.0)
                            quarter = 0.25 * g
                            field[(0,) + at] = (
                                held * (old_x + coriolis * old_y)
                                + quarter * force_x
                                + stat[(2,) + beside]
                            )
                            field[(1,) + at] = (
                                held * (old_y - coriolis * old_x)
                                + quarter * force_y
                                + stat[(3,) + beside]
                            )
                    for i in range(GROUP):
                        here = column[i + 1]
                        new_x = field[0, here, pl.ds(rows + low_off, 8), :]
                        new_y = field[1, here, pl.ds(rows + low_off, 8), :]
                        lanes = pl.ds(pl.multiple_of(column[i] * LANES, LANES), LANES)
                        total[0, :, lanes] += new_x
                        total[1, :, lanes] += new_y
                        total[2, :, lanes] += jnp.sqrt(1.0 + new_x * new_x + new_y * new_y)

                over_tiles(stress)
                over_tiles(speed)

            for c in range(tiles):
                lanes = slice(c * LANES, (c + 1) * LANES)
                mine = [field[p, c + 1, low_off + rows : low_off + 2 * rows, :] for p in range(5)]
                if last:
                    mine[2:] = [
                        0.5 * (mine[2] + mine[3]),
                        0.5 * (mine[2] - mine[3]),
                        0.5 * mine[4],
                    ]
                    for part in range(2):
                        total[part, :, lanes] = (
                            total[part, :, lanes] * (1.0 / SUBCYCLES) - extra[part, :, lanes]
                        )
                    total[2, :, lanes] = (
                        total[2, :, lanes] * extra[2, :, lanes] * (1.0 / SUBCYCLES)
                    )
                for p in range(5):
                    out[p, :, lanes] = mine[p]

        def ocean():
            if first:
                load_windows(stat, [(plane, 5 + plane) for plane in range(2)], (0, 0))
            if not ocean_active:
                out[...] = own[:5]
                return
            load_windows(field, [(plane, plane) for plane in range(5)], (low_off, 1))
            for plane in range(5):
                for ref in (field, other):
                    ref[plane, 0] = zero_column
                    ref[plane, tiles + 1] = zero_column

            for turn in range(OCEAN_DEPTH):
                source, target = (field, other) if turn % 2 == 0 else (other, field)
                row_spans = spans(turn + 1)

                def advect(group, column):
                    for span in row_spans:
                        row = span + low_off
                        pos_x, neg_x, pos_y, neg_y = [], [], [], []
                        for i in range(GROUP):
                            beside = (column[i], pl.ds(span, 8), slice(None))
                            ux = courant * stat[(0,) + beside]
                            uy = courant * stat[(1,) + beside]
                            pos_x.append(jnp.maximum(ux, 0.0))
                            neg_x.append(jnp.minimum(ux, 0.0))
                            pos_y.append(jnp.maximum(uy, 0.0))
                            neg_y.append(jnp.minimum(uy, 0.0))
                        for level in range(5):
                            side = sides(source, level, column, row, {})
                            for i in range(GROUP):
                                here = column[i + 1]
                                left, right = side(i)
                                centre = source[level, here, pl.ds(row, 8), :]
                                below = source[level, here, pl.ds(row - 1, 8), :]
                                above = source[level, here, pl.ds(row + 1, 8), :]
                                change = (
                                    pos_x[i] * (centre - below)
                                    + neg_x[i] * (above - centre)
                                    + pos_y[i] * (centre - left)
                                    + neg_y[i] * (right - centre)
                                )
                                if level:
                                    change = level_speed[level] * change
                                target[level, here, pl.ds(row, 8), :] = centre - change

                over_tiles(advect)

            done = field if OCEAN_DEPTH % 2 == 0 else other
            for p in range(5):
                for c in range(tiles):
                    out[p, :, c * LANES : (c + 1) * LANES] = done[
                        p, c + 1, low_off + rows : low_off + 2 * rows, :
                    ]

        @pl.when(flag[0] < strips)
        def _():
            ice()

        @pl.when(flag[0] >= strips)
        def _():
            ocean()

    return kernel


WIDE = 256


def scatter_half(half, values, spots_of, weights_of, sums, blocks, rights=None):
    rows = values.shape[1]
    columns = values.shape[2]
    groups = columns // WIDE
    spots = rows * groups
    turns = 2 * rows
    sums[...] = jnp.zeros_like(sums)
    high_at = lax.broadcasted_iota(jnp.int32, (spots, columns), 0).astype(jnp.bfloat16)
    low_at = lax.broadcasted_iota(jnp.int32, (WIDE, columns), 0).astype(jnp.bfloat16)
    zero = jnp.zeros((), jnp.bfloat16)
    one = jnp.ones((), jnp.bfloat16)

    def build(turn, left, right=None):
        entry = turn // rows
        row = turn % rows
        spot = spots_of[entry, pl.ds(row, 1), :].astype(jnp.int32)
        scale = weights_of[entry, pl.ds(row, 1), :].astype(jnp.float32) / weight_norm
        low = jnp.bitwise_and(spot, WIDE - 1)
        high = jnp.right_shift(spot, 8) - half * spots
        inside = jnp.logical_and(high >= 0, high < spots)
        place = jnp.bitwise_and(high, groups - 1) * rows + high // groups
        place = jnp.where(inside, place, -1)
        place = place.astype(jnp.float32).astype(jnp.bfloat16)
        if right is not None:
            low = low.astype(jnp.float32).astype(jnp.bfloat16)
            right[...] = jnp.where(low_at == low, one, zero)
        hit = high_at == place
        for channel in range(3):
            value = values[channel, pl.ds(row, 1), :] * scale
            coarse = value.astype(jnp.bfloat16)
            fine = (value - coarse.astype(jnp.float32)).astype(jnp.bfloat16)
            for part, piece in enumerate((coarse, fine)):
                first = (2 * channel + part) * spots
                left[first : first + spots, :] = jnp.where(hit, piece, zero)

    def multiply(left, right):
        sums[...] += lax.dot_general(
            left[...],
            right[...],
            (((1,), (1,)), ((), ())),
            preferred_element_type=jnp.float32,
        )

    if rights is None:
        left_a, right_a, left_b, right_b = blocks
    else:
        left_a, left_b = blocks
        right_a = right_b = None

    def at(turn, right):
        return right if rights is None else rights.at[turn]

    build(0, left_a, right_a)

    def step(pair, carry):
        build(2 * pair + 1, left_b, right_b)
        multiply(left_a, at(2 * pair, right_a))
        build(jnp.minimum(2 * pair + 2, turns - 1), left_a, right_a)
        multiply(left_b, at(2 * pair + 1, right_b))
        return carry

    lax.fori_loop(0, turns // 2, step, 0)

    def tile(channel, group):
        first = 2 * channel * spots + group * rows
        return sums[first : first + rows, :] + sums[first + spots : first + spots + rows, :]

    return tile, groups


def write_half(half, values, spots_of, weights_of, out, sums, blocks, rights=None):
    tile, groups = scatter_half(half, values, spots_of, weights_of, sums, blocks, rights)
    for channel in range(3):
        for g in range(groups):
            out[channel, :, g * WIDE : (g + 1) * WIDE] = tile(channel, g)


def lower_kernel(strips, flag, average, targets, weights, out, sums, *blocks):
    @pl.when(flag[0] < strips)
    def _():
        write_half(0, average, targets, weights, out, sums, blocks)


def rights_kernel(strips, flag, links, out):
    @pl.when(flag[0] >= strips)
    def _():
        turns, _, columns = out.shape
        rows = turns // 2
        low_at = lax.broadcasted_iota(jnp.int32, (WIDE, columns), 0).astype(jnp.bfloat16)

        def step(turn, carry):
            spot = links[turn // rows, pl.ds(turn % rows, 1), :].astype(jnp.int32)
            low = jnp.bitwise_and(spot, WIDE - 1).astype(jnp.float32).astype(jnp.bfloat16)
            out[turn] = jnp.where(
                low_at == low, jnp.ones((), jnp.bfloat16), jnp.zeros((), jnp.bfloat16)
            )
            return carry

        lax.fori_loop(0, turns, step, 0)


def upper_kernel(strips, flag, before, links, rights, out, sums, *blocks):
    @pl.when(flag[0] >= strips)
    def _():
        write_half(1, before, links.at[:2], links.at[2:], out, sums, blocks, rights)


def final_kernel(strips, flag, fields, average, lower, upper, state, coupled):
    @pl.when(flag[0] < strips)
    def _():
        state[0] = fields[...]
        coupled[0] = average[...]

    @pl.when(flag[0] >= strips)
    def _():
        flux = lower[...] + upper[...]
        coupled[0] = flux
        state[0, 0] = fields[0] - dilution * flux[2]
        state[0, 1:] = fields[1:]


def body(initial, ice_forcing, ocean_current, ice_cover, targets, weights):
    rows, columns = initial.shape[2:]
    tiles = columns // LANES
    strips = lax.axis_size("blk")
    both = ("comp", "blk")
    flag = lax.axis_index(both).astype(jnp.int32).reshape(1)

    def swapped(value, kinds, start):
        pairs = [
            (kind * strips + source, kind * strips + target)
            for kind in kinds
            for b in range(start, strips - 1, 2)
            for source, target in ((b, b + 1), (b + 1, b))
        ]
        return lax.ppermute(value, both, pairs)

    def shape(*dims):
        return pltpu.VMEM(dims, jnp.float32)

    def held(*values):
        return [pltpu.with_memory_space_constraint(value, pltpu.VMEM) for value in values]

    inputs = (initial, ice_forcing, ocean_current, ice_cover, targets, weights)
    block, extra = pl.pallas_call(
        partial(prep_kernel, strips),
        compiler_params=LIMITED,
        out_shape=[shape(9, rows, columns), shape(4, rows, columns)],
        in_specs=[SMEM] + [pl.BlockSpec(memory_space=pltpu.HBM)] * 6,
        out_specs=[VMEM] * 2,
        scratch_shapes=[pltpu.VMEM(value.shape, value.dtype) for value in inputs]
        + [pltpu.SemaphoreType.DMA((6,))],
    )(flag, *(pltpu.with_memory_space_constraint(value, pltpu.HBM) for value in inputs))

    rounds = SUBCYCLES // ICE_DEPTH
    each = OCEAN_DEPTH // ICE_DEPTH
    window = 3 * rows
    stat = total = None
    for turn in range(rounds):
        first, last = turn == 0, turn == rounds - 1
        active = turn % each == 0
        kinds = (0, 1) if active else (0,)
        near = swapped(block, kinds, 0)
        far = swapped(block, kinds, 1)
        operands = [flag, block, far, near]
        outs = [shape(5, rows, columns), shape(3, rows, columns)]
        if not first:
            operands += [stat, total]
        if last:
            operands.append(extra)
        if first:
            outs.append(shape(4, tiles, window, LANES))
        done = pl.pallas_call(
            make_round(strips, first, last, active, rows, tiles),
            compiler_params=LIMITED,
            out_shape=outs,
            in_specs=[SMEM] + [VMEM] * (len(operands) - 1),
            out_specs=[VMEM] * len(outs),
            scratch_shapes=[pltpu.VMEM((5, tiles + 2, window + 2 * PAD, LANES), jnp.float32)] * 2,
        )(flag, *held(*operands[1:]))
        block, total = done[:2]
        if first:
            stat = done[2]

    average = total
    links_before = lax.ppermute(
        extra, both, [(strips + b, strips + (b + 1) % strips) for b in range(strips)]
    )
    before = lax.ppermute(average, both, [(b, strips + (b + 1) % strips) for b in range(strips)])
    spots = rows * columns // WIDE
    sums = pltpu.VMEM((6 * spots, WIDE), jnp.float32)
    left = pltpu.VMEM((6 * spots, columns), jnp.bfloat16)
    right = pltpu.VMEM((WIDE, columns), jnp.bfloat16)

    def scattered(kernel, scratch, *operands):
        return pl.pallas_call(
            partial(kernel, strips),
            compiler_params=LIMITED,
            out_shape=shape(3, rows, columns),
            in_specs=[SMEM] + [VMEM] * len(operands),
            out_specs=VMEM,
            scratch_shapes=scratch,
        )(flag, *held(*operands))

    lower = scattered(lower_kernel, [sums, left, right, left, right], average, targets, weights)
    received = lax.ppermute(lower, both, [(b, strips + b) for b in range(strips)])
    rights = pl.pallas_call(
        partial(rights_kernel, strips),
        compiler_params=LIMITED,
        out_shape=pltpu.VMEM((2 * rows, WIDE, columns), jnp.bfloat16),
        in_specs=[SMEM, VMEM],
        out_specs=VMEM,
    )(flag, *held(links_before))
    upper = scattered(upper_kernel, [sums, left, left], before, links_before, rights)
    return tuple(
        pl.pallas_call(
            partial(final_kernel, strips),
            compiler_params=LIMITED,
            out_shape=[
                jax.ShapeDtypeStruct((1, 5, rows, columns), jnp.float32),
                jax.ShapeDtypeStruct((1, 3, rows, columns), jnp.float32),
            ],
            in_specs=[SMEM] + [VMEM] * 4,
            out_specs=[VMEM] * 2,
        )(flag, *held(block, average, received, upper))
    )


def solution(mesh):
    placed = (
        P("comp", None, "blk", None),
        P(None, "blk", None),
        P(None, "blk", None),
        P("blk", None),
        P(None, "blk", None),
        P(None, "blk", None),
    )
    return jax.shard_map(
        body,
        mesh=mesh,
        in_specs=placed,
        out_specs=(P("comp", None, "blk", None), P("comp", None, "blk", None)),
        check_vma=False,
    )
```
